32 devices in a mesh: context: 2 (over core), tensor: 4 (over y, x), fsdp: 4 (over z).
Axes of the slice: x: 2, y: 2, z: 4, core: 2. Of those that a mesh axis runs over, the one named last changes fastest.
Arguments:
- input_raw: bfloat16 [4, 1024, 5120], P('fsdp', ('context', 'tensor')), may hold values from -6 to 6
- state_proj_raw: bfloat16 [4, 1024, 256], P('fsdp', ('context', 'tensor')), may hold values from -6 to 6
- gate_branch: bfloat16 [4, 1024, 5120], P('fsdp', ('context', 'tensor')), may hold values from -6 to 6
- step_raw: bfloat16 [4, 1024, 80], P('fsdp', ('context', 'tensor')), may hold values from -6 to 6
- convolution_taps: float32 [4, 5376], replicated, may hold values from -3 to 3
- convolution_bias: float32 [5376], replicated, may hold values from -3 to 3
- step_bias: float32 [80], P('tensor'), may hold values from -1.5 to 0.5
- decay_log_rate: float32 [80], P('tensor'), may hold values from -13 to -2, as said below
- skip_weight: float32 [80], P('tensor'), may hold values from 0.5 to 2
- gated_norm_gain: float32 [5120], P('tensor'), may hold values from 0.1 to 1.9
- output_weight: bfloat16 [5120, 2560], P('tensor', 'fsdp'), may hold values from -0.078125 to 0.078125
- adapter_down: bfloat16 [5120, 16], P('tensor'), may hold values from -0.078125 to 0.078125
- adapter_up: bfloat16 [16, 2560], replicated, may hold values from -0.29882812 to 0.29882812
- cotangent: bfloat16 [4, 1024, 2560], P('fsdp', ('context', 'tensor')), may hold values from -6 to 6
Outputs:
- mixed: bfloat16 [4, 1024, 2560], P('fsdp', ('context', 'tensor'))
- grad_a: float32 [5120, 16], P('tensor')
- grad_b: float32 [16, 2560], replicated
The draws below stay inside these ranges and needn't reach their ends.
Inputs may be any that keep to these rules, and one draw needn't show every extreme that they name: `decay_log_rate`: logarithms of positive decay rates.
All inputs are finite; a program needn't handle non-finite values.
Results may differ from the reference program's by a relative error of at most 0.017.
Values may be sent and summed in bfloat16 or wider, within the bound.
A program may use at most 128 MiB of HBM per device.

```python
import math
import jax
import jax.numpy as jnp
from jax import lax

MODEL_WIDTH = 2560
H = 80
N = 128
ADAPTER_RANK = 16
CONV = 4
MIXER_WIDTH = 5120
SEQS = 4
LEN = 1024


def draw_decay_log_rate(key, part):
    pick_key, slow_key, fast_key = jax.random.split(jax.random.fold_in(key, 11), 3)
    keep_share = 5
    slow_mask = jax.random.randint(pick_key, (H,), 0, 10) < keep_share
    low_log = jnp.log(0.5 / LEN)
    high_log = jnp.log(2.5 / LEN)
    slow_rate = jax.random.uniform(slow_key, (H,), jnp.float32, low_log, high_log)
    fast_rate = jnp.log(jax.random.uniform(fast_key, (H,), jnp.float32, 1.0 / 60.0, 1.0 / 20.0))
    return jnp.where(slow_mask, slow_rate, fast_rate)


def block_levels(rng, dims, cuts, low, largest):
    gain, own = 1.0, jax.random.fold_in(rng, 6)
    for position, parts in cuts:
        heights = jnp.exp(jax.random.uniform(jax.random.fold_in(own, position), (parts,), jnp.float32, low / len(cuts), largest / len(cuts)))
        gain = gain * jnp.repeat(heights, dims[position] // parts).reshape([-1 if axis == position else 1 for axis in range(len(dims))])
    return gain


def centred(stream_key, dims, width, reach, cuts=(), held_as=jnp.bfloat16):
    level = block_levels(stream_key, dims, cuts, -0.22, 0.18) if cuts else 1.0
    result = jax.random.normal(stream_key, dims, jnp.float32) * width * level
    return jnp.minimum(jnp.maximum(result, -reach), reach).astype(held_as)


def setup_inputs(seed: int = 0) -> dict:
    arg_keys = jax.random.split(jax.random.key(seed), 15)
    input_raw = centred(arg_keys[0], (SEQS, LEN, MIXER_WIDTH), 1.0, 6.0, ((0, 4), (1, 8)))
    state_proj_raw = centred(arg_keys[1], (SEQS, LEN, 2 * N), 1.0, 6.0, ((0, 4), (1, 8)))
    gate_branch = centred(arg_keys[2], (SEQS, LEN, MIXER_WIDTH), 1.0, 6.0, ((0, 4), (1, 8)))
    step_raw = centred(arg_keys[3], (SEQS, LEN, H), 1.0, 6.0, ((0, 4), (1, 8)))
    convolution_taps = centred(arg_keys[4], (CONV, MIXER_WIDTH + 2 * N), CONV ** -0.5, 3.0, (), jnp.float32)
    convolution_bias = centred(arg_keys[5], (MIXER_WIDTH + 2 * N,), 0.5, 3.0, (), jnp.float32)
    step_bias = jnp.clip(-1.5 + 2.0 * jax.random.uniform(arg_keys[6], (H,), jnp.float32) ** block_levels(arg_keys[6], (H,), ((0, 4),), -0.2, 0.2), -1.5, 0.5)
    decay_log_rate = draw_decay_log_rate(jax.random.fold_in(arg_keys[14], 71), 0)
    skip_weight = jnp.clip(0.5 + 1.5 * jax.random.uniform(arg_keys[8], (H,), jnp.float32) ** block_levels(arg_keys[8], (H,), ((0, 4),), -0.2, 0.2), 0.5, 2.0)
    gated_norm_gain = jnp.clip(1.0 + 0.18 * jax.random.normal(arg_keys[9], (MIXER_WIDTH,), jnp.float32), 0.1, 1.9)
    output_weight = centred(arg_keys[10], (MIXER_WIDTH, MODEL_WIDTH), MIXER_WIDTH ** -0.5, 0.078125, ((0, 4), (1, 4)))
    adapter_down = centred(arg_keys[11], (MIXER_WIDTH, ADAPTER_RANK), MIXER_WIDTH ** -0.5, 0.078125, ((0, 4),))
    adapter_up = centred(arg_keys[12], (ADAPTER_RANK, MODEL_WIDTH), 0.05, 0.29882812)
    cotangent = centred(arg_keys[13], (SEQS, LEN, MODEL_WIDTH), 1.0, 6.0, ((0, 4), (1, 8)))
    return dict(input_raw=input_raw, state_proj_raw=state_proj_raw, gate_branch=gate_branch, step_raw=step_raw, convolution_taps=convolution_taps, convolution_bias=convolution_bias, step_bias=step_bias, decay_log_rate=decay_log_rate, skip_weight=skip_weight, gated_norm_gain=gated_norm_gain, output_weight=output_weight, adapter_down=adapter_down, adapter_up=adapter_up, cotangent=cotangent)


def ssd_blocks(x_heads, b_rows, c_rows, step_size, log_decay, block_len):
    highest = lax.Precision.HIGHEST
    length = x_heads.shape[0]
    head_count = x_heads.shape[1]
    head_size = x_heads.shape[2]
    state_size = b_rows.shape[1]
    blocks = length // block_len
    causal = jnp.arange(block_len)[:, None] >= jnp.arange(block_len)[None, :]

    def advance(state_now, pieces):
        x_block, b_block, c_block, step_block, decay_block = pieces
        cum_decay = jnp.cumsum(decay_block, axis=0)
        cum_heads = cum_decay.T
        gap_decay = cum_heads[:, :, None] - cum_heads[:, None, :]
        decay_mat = jnp.where(causal[None], jnp.exp(jnp.where(causal[None], gap_decay, 0.0)), 0.0)
        gram_mat = jnp.dot(c_block, b_block.T, precision=highest)
        x_scaled = x_block * step_block[:, :, None]
        y_inner = jnp.einsum('hij,jhp->ihp', decay_mat * gram_mat[None], x_scaled, precision=highest)
        y_state = jnp.exp(cum_decay)[:, :, None] * jnp.einsum('in,hpn->ihp', c_block, state_now, precision=highest)
        tail_decay = jnp.exp(cum_decay[-1][None, :] - cum_decay)
        state_next = jnp.exp(cum_decay[-1])[:, None, None] * state_now + jnp.einsum('jhp,jn->hpn', x_scaled * tail_decay[:, :, None], b_block, precision=highest)
        return (state_next, y_inner + y_state)
    start_state = jnp.zeros((head_count, head_size, state_size), jnp.float32)
    state_end, y_blocks = lax.scan(advance, start_state, (x_heads.reshape(blocks, block_len, head_count, head_size), b_rows.reshape(blocks, block_len, state_size), c_rows.reshape(blocks, block_len, state_size), step_size.reshape(blocks, block_len, head_count), log_decay.reshape(blocks, block_len, head_count)))
    return (y_blocks.reshape(length, head_count, head_size), state_end)

def reference(input_raw, state_proj_raw, gate_branch, step_raw, convolution_taps, convolution_bias, step_bias, decay_log_rate, skip_weight, gated_norm_gain, output_weight, adapter_down, adapter_up, cotangent):
    highest = lax.Precision.HIGHEST
    inner_width = input_raw.shape[2]
    state_size = state_proj_raw.shape[2] // 2
    head_count = decay_log_rate.shape[0]
    head_size = inner_width // head_count
    length = input_raw.shape[1]
    taps = convolution_taps.shape[0]
    block_len = math.gcd(length, 256)
    lowrank_factor = 2.0 / math.sqrt(input_raw.shape[0] * length)
    decay_rate = jnp.exp(decay_log_rate)

    def one_sequence(pieces):
        x_seq, bc_seq, z_seq, dt_seq, cotangent_sequence = pieces
        joined = jnp.concatenate([x_seq, bc_seq], axis=1)
        padded = jnp.concatenate([jnp.zeros((taps - 1, joined.shape[1]), joined.dtype), joined], axis=0)
        pre_act = convolution_bias[None, :] + convolution_taps[0][None, :] * padded[0:length].astype(jnp.float32)
        for tap_index in range(1, taps):
            pre_act = pre_act + convolution_taps[tap_index][None, :] * padded[tap_index:tap_index + length].astype(jnp.float32)
        xbc = jax.nn.silu(pre_act).astype(jnp.bfloat16)
        x_heads = xbc[:, :inner_width].astype(jnp.float32).reshape(length, head_count, head_size)
        b_rows = xbc[:, inner_width:inner_width + state_size].astype(jnp.float32)
        c_rows = xbc[:, inner_width + state_size:].astype(jnp.float32)
        step_size = jax.nn.softplus(dt_seq.astype(jnp.float32) + step_bias[None, :])
        log_decay = -step_size * decay_rate[None, :]
        y_heads, state_end = ssd_blocks(x_heads, b_rows, c_rows, step_size, log_decay, block_len)
        y_heads = y_heads + skip_weight[None, :, None] * x_heads
        gated = y_heads.reshape(length, inner_width) * jax.nn.silu(z_seq.astype(jnp.float32))
        row_norm_scale = lax.rsqrt(lax.optimization_barrier(jnp.mean(gated * gated, axis=1)) + 1e-05)
        gated_output = (gated * gated_norm_gain[None, :]).astype(jnp.bfloat16)
        adapter_branch = jnp.dot(gated_output, adapter_down, preferred_element_type=jnp.float32).astype(jnp.bfloat16)
        frozen_piece = jnp.dot(gated_output, output_weight, preferred_element_type=jnp.float32)
        frozen_piece = frozen_piece + 2.0 * jnp.dot(adapter_branch, adapter_up, preferred_element_type=jnp.float32)
        mixed = (row_norm_scale[:, None] * frozen_piece).astype(jnp.bfloat16)
        weighted = lowrank_factor * row_norm_scale[:, None] * adapter_branch.astype(jnp.float32)
        grad_b_part = jnp.dot(weighted.T, cotangent_sequence.astype(jnp.float32), precision=highest)
        adapter_gradient = lowrank_factor * row_norm_scale[:, None] * jnp.dot(cotangent_sequence, adapter_up.T, preferred_element_type=jnp.float32)
        grad_a_part = jnp.dot(gated_output.astype(jnp.float32).T, adapter_gradient, precision=highest)
        return (mixed, grad_a_part, grad_b_part)
    mixed, grad_a_parts, grad_b_parts = lax.map(one_sequence, (input_raw, state_proj_raw, gate_branch, step_raw, cotangent))
    return (mixed, lax.optimization_barrier(jnp.sum(grad_a_parts, axis=0)), lax.optimization_barrier(jnp.sum(grad_b_parts, axis=0)))
```

```python
import functools
import math

import jax
import jax.numpy as jnp
from jax import lax
from jax.experimental import pallas as pl
from jax.experimental.pallas import tpu as pltpu
from jax.sharding import PartitionSpec as P

EPS = 1e-05
MESH = pl.DeviceIdType.MESH
HI = lax.Precision.HIGHEST
BF = jnp.bfloat16
F32 = jnp.float32


def dot(a, b, ca=1, cb=0, precision=None):
    return lax.dot_general(
        a, b, (((ca,), (cb,)), ((), ())), preferred_element_type=F32, precision=precision
    )


def iota(shape, dim):
    return lax.broadcasted_iota(jnp.int32, shape, dim)


def kernel(
    nt, nf, nc, hl,
    x_ref, bc_ref, z_ref, dt_ref, taps_ref, bias_ref, hp_ref, gain_ref, w_ref, down_ref, up_ref, cot_ref,
    mixed_ref, ga_ref, gb_ref,
    halo_x, halo_bc, x_send, x_all, z_all, bc_all, dt_all, wbuf, a_s, step_s, at_s, stept_s,
    stl, msg, st_in, inc_s, e_s, y_s, g_s, adx, ad_in, ag_own, ag_all, gb_own, gb_in, comb, comb_c, comb2, comb_f,
    fin, rs_send, rs_recv,
    h_ss, h_rs, dt_ss, dt_rs, bc_ss, bc_rs, x_ss, x_rs, z_ss, z_rs, w_ss, w_rs, wf_ss, wf_rs, st_ss, st_rs,
    ad_ss, ad_rs, ag_ss, ag_rs, ga_ss, ga_rs, cc_ss, cc_rs, cf_ss, cf_rs, fin_ss, fin_rs, r_ss, r_rs, loc,
):
    t = lax.axis_index("tensor")
    f = lax.axis_index("fsdp")
    c = lax.axis_index("context")
    L = x_ref.shape[0]
    LW = x_all.shape[1]
    W = w_ref.shape[1]
    N = bc_ref.shape[1] // 2
    R = w_ref.shape[0] // nc
    HS = LW // hl
    idx = c * nt + t
    total = nc * nt

    def tp(e):
        return lax.rem(t + e, nt)

    def place(i):
        return {"context": i // nt, "tensor": lax.rem(i, nt)}

    def copy(src, dst, ss, rs, dev):
        cp = pltpu.make_async_remote_copy(
            src_ref=src, dst_ref=dst, send_sem=ss, recv_sem=rs, device_id=dev, device_id_type=MESH
        )
        cp.start()
        return cp

    nxt, prv = lax.rem(idx + 1, total), lax.rem(idx + total - 1, total)
    bar = pltpu.get_barrier_semaphore()
    greet = [{"tensor": tp(e)} for e in range(1, nt)]
    greet += [{"fsdp": lax.rem(f + d, nf)} for d in range(1, nf)]
    greet += [{"context": lax.rem(c + k, nc)} for k in range(1, nc)]
    greet += [place(nxt), place(prv)]
    for dev in greet:
        pl.semaphore_signal(bar, inc=1, device_id=dev, device_id_type=MESH)
    pl.semaphore_wait(bar, len(greet))
    sent = []

    h1 = copy(x_ref.at[L - 16 : L, :], halo_x, h_ss.at[0], h_rs.at[0], place(nxt))
    h2 = copy(bc_ref.at[L - 16 : L, :], halo_bc, h_ss.at[1], h_rs.at[1], place(nxt))
    own_rows = pl.ds(pl.multiple_of(t * L, L), L)
    dts = [copy(dt_ref, dt_all.at[own_rows, :], dt_ss.at[e], dt_rs.at[e], {"tensor": tp(e)}) for e in range(1, nt)]
    share = pl.ds(pl.multiple_of(c * R, 16), R)
    ws = [
        copy(w_ref.at[share, :], wbuf.at[d, share, :], w_ss.at[d], w_rs.at[d], {"fsdp": lax.rem(f + d, nf)})
        for d in range(1, nf)
    ]
    own_w = pltpu.make_async_copy(w_ref, wbuf.at[0], loc.at[0])
    own_w.start()
    own_cols = pl.ds(pl.multiple_of(t * LW, 128), LW)
    own_z = pltpu.make_async_copy(z_ref.at[:, own_cols], z_all.at[own_rows, :], loc.at[1])
    own_z.start()
    dt_all[own_rows, :] = dt_ref[...]

    h1.wait()
    h2.wait()
    live = (idx > 0).astype(F32)

    def conv(src, halo, col, tap_col):
        lanes = pl.ds(col, 128)
        wide = pl.ds(tap_col, 128)
        ext = jnp.concatenate([halo[8:16, lanes].astype(F32) * live, src[:, lanes].astype(F32)], axis=0)
        acc = bias_ref[:, wide] + taps_ref[0:1, wide] * ext[5 : 5 + L]
        for k in range(1, 4):
            acc = acc + taps_ref[k : k + 1, wide] * ext[5 + k : 5 + k + L]
        return (acc / (1.0 + jnp.exp(-acc))).astype(BF)

    wide0 = x_ref.shape[1]
    for j in range(2 * N // 128):
        bc_all[own_rows, j * 128 : (j + 1) * 128] = conv(bc_ref, halo_bc, j * 128, wide0 + j * 128)
    bcs = [
        copy(bc_all.at[own_rows, :], bc_all.at[own_rows, :], bc_ss.at[e], bc_rs.at[e], {"tensor": tp(e)})
        for e in range(1, nt)
    ]
    xs, zs = [], []

    def conv_group(e, store):
        base = tp(e) * LW

        def lap(j, carry):
            col = pl.multiple_of(base + j * 128, 128)
            store(pl.ds(pl.multiple_of(j * 128, 128), 128), conv(x_ref, halo_x, col, col))
            return carry

        lax.fori_loop(0, LW // 128, lap, 0)

    for e in range(1, nt):
        def put(lanes, val, e=e):
            x_send[e - 1, :, lanes] = val

        conv_group(e, put)
        xs.append(copy(x_send.at[e - 1], x_all.at[own_rows, :], x_ss.at[e], x_rs.at[e], {"tensor": tp(e)}))
    for e in range(1, nt):
        cols = pl.ds(pl.multiple_of(tp(e) * LW, 128), LW)
        zs.append(copy(z_ref.at[:, cols], z_all.at[own_rows, :], z_ss.at[e], z_rs.at[e], {"tensor": tp(e)}))

    def put_own(lanes, val):
        x_all[own_rows, lanes] = val

    conv_group(0, put_own)
    e_s[...] = (iota((128, LW), 1) // HS == iota((128, LW), 0)).astype(F32)
    spread16 = e_s[...].astype(BF)

    def spread(rows):
        return dot(jnp.broadcast_to(rows, (8, 128)), e_s[...], precision=HI)

    for cp in dts:
        cp.wait()
    HR = at_s.shape[1]
    sel = ((iota((128, 128), 0) == iota((128, 128), 1) + t * hl) & (iota((128, 128), 1) < hl)).astype(BF)
    sel_t = ((iota((HR, 128), 1) == iota((HR, 128), 0) + t * hl) & (iota((HR, 128), 0) < hl)).astype(BF)
    eye = (iota((HR, 128), 0) == iota((HR, 128), 1)).astype(F32)
    hp = hp_ref[...]
    hp_t = dot(eye, hp, 1, 1, HI)
    tri = (iota((L, L), 0) >= iota((L, L), 1)).astype(F32)

    def softplus(v):
        return jnp.maximum(v, 0.0) + jnp.log1p(jnp.exp(-jnp.abs(v)))

    for b in range(nt):
        rows = slice(b * L, (b + 1) * L)
        raw = dt_all[rows, :]
        step = softplus(dot(raw, sel) + hp[0:1, :])
        step_s[rows, :] = step
        a_s[rows, :] = dot(tri, -step * jnp.exp(hp[1:2, :]), precision=HI)
        step_t = softplus(dot(sel_t, raw, 1, 1) + hp_t[:, 0:1])
        stept_s[b] = step_t
        at_s[b] = dot(-step_t * jnp.exp(hp_t[:, 1:2]), tri, 1, 1, HI)
    for cp in bcs:
        cp.wait()
    for cp in xs:
        cp.wait()

    state = jnp.zeros((N, LW), F32)
    before = jnp.zeros((1, 128), F32)
    for b in range(nt):
        rows = slice(b * L, (b + 1) * L)
        stl[b, 0:N, :] = state
        stl[b, N : N + 8, :] = spread(jnp.exp(before))
        a = a_s[rows, :]
        last = a[L - 1 : L, :]
        weight = (jnp.exp(last - a) * step_s[rows, :]).astype(BF)
        xw = (x_all[rows, :].astype(F32) * dot(weight, spread16)).astype(BF)
        state = spread(jnp.exp(last))[0:1, :] * state + dot(bc_all[rows, 0:N], xw, 0, 0)
        before = before + last
    msg[0:N, :] = state
    msg[N : N + 8, :] = spread(before)
    sts = [
        copy(msg, st_in.at[c], st_ss.at[k], st_rs.at[k], {"context": lax.rem(c + k, nc)})
        for k in range(1, nc)
    ]

    left = iota((L, 2 * HS), 1) < HS

    def inner(b, carry):
        rows = pl.ds(pl.multiple_of(b * L, L), L)
        gram = dot(bc_all[rows, N : 2 * N], bc_all[rows, 0:N], 1, 1)
        gram = jnp.where(iota((L, L), 0) >= iota((L, L), 1), gram, 0.0)
        a = a_s[rows, :]
        at = at_s[b]
        stt = stept_s[b]
        for pair in range(hl // 2):
            lanes = slice(pair * 2 * HS, (pair + 1) * 2 * HS)
            xp = x_all[rows, lanes]
            out = []
            for h in (2 * pair, 2 * pair + 1):
                gap = jnp.minimum(a[:, h : h + 1] - at[h : h + 1, :], 0.0)
                m = (jnp.exp(gap) * gram * stt[h : h + 1, :]).astype(BF)
                out.append(dot(m, xp))
            y_s[rows, lanes] = jnp.where(left, out[0], out[1])
        return carry

    lax.fori_loop(0, nt, inner, 0)

    for cp in sts:
        cp.wait()
    inc_s[...] = jnp.zeros_like(inc_s)

    def chain(k, carry):
        inc_s[...] = jnp.exp(st_in[k, N : N + 1, :]) * inc_s[...] + st_in[k, 0:N, :]
        return carry

    lax.fori_loop(0, c, chain, 0)
    for cp in zs:
        cp.wait()
    own_z.wait()
    skip = spread(hp[2:3, :])[0:1, :]
    ones = jnp.ones((8, LW), BF)

    def gate(b, carry):
        rows = pl.ds(pl.multiple_of(b * L, L), L)
        start = (stl[b, 0:N, :] + stl[b, N : N + 1, :] * inc_s[...]).astype(BF)
        reach = dot(jnp.exp(a_s[rows, :]).astype(BF), spread16)
        y = y_s[rows, :] + reach * dot(bc_all[rows, N : 2 * N], start)
        y = y + skip * x_all[rows, :].astype(F32)
        z = z_all[rows, :].astype(F32)
        g = y * (z / (1.0 + jnp.exp(-z)))
        out = (g * gain_ref[...]).astype(BF)
        g_s[rows, :] = out
        adx[b, 0:16, :] = dot(down_ref[...], out, 1, 1)
        adx[b, 16:24, :] = dot(ones, (g * g).astype(BF), 1, 1)
        return carry

    lax.fori_loop(0, nt, gate, 0)
    ads = [copy(adx.at[tp(e)], ad_in.at[e], ad_ss.at[e], ad_rs.at[e], {"tensor": tp(e)}) for e in range(1, nt)]

    half = (nt * L) // 2

    def project(d):
        def lap(i, carry):
            rows = pl.ds(pl.multiple_of(i * half, half), half)
            rs_send[d, rows, :] = dot(g_s[rows, :], wbuf[d]).astype(BF)
            return carry

        lax.fori_loop(0, 2, lap, 0)

    def scatter(d):
        return [
            copy(
                rs_send.at[d, pl.ds(pl.multiple_of(tp(e) * L, L), L), :],
                rs_recv.at[d, e - 1], r_ss.at[d, e], r_rs.at[d, e], {"tensor": tp(e)},
            )
            for e in range(1, nt)
        ]

    own_w.wait()
    project(0)
    for cp in ads:
        cp.wait()
    red = adx[t]
    for e in range(1, nt):
        red = red + ad_in[e]
    scale_row = lax.rsqrt(red[16:17, :] / (LW * nt) + EPS)
    ad16 = red[0:16, :].astype(BF)
    factor = 2.0 / math.sqrt(L * nt * nc * nf)
    cot = cot_ref[...]
    ag_own[...] = factor * scale_row * dot(up_ref[...], cot, 1, 1)
    ags = [copy(ag_own, ag_all.at[t], ag_ss.at[e], ag_rs.at[e], {"tensor": tp(e)}) for e in range(1, nt)]
    gb_own[...] = dot((factor * scale_row * ad16.astype(F32)).astype(BF), cot)
    part = gb_own.shape[1] // nt
    own_part = pl.ds(pl.multiple_of(t * part, 128), part)
    gbs = [
        copy(
            gb_own.at[:, pl.ds(pl.multiple_of(tp(e) * part, 128), part)],
            gb_in.at[e], ga_ss.at[e], ga_rs.at[e], {"tensor": tp(e)},
        )
        for e in range(1, nt)
    ]
    sent += scatter(0)
    wfs = []
    for d in range(1, nf):
        ws[d - 1].wait()
        wfs.append([
            copy(wbuf.at[d, share, :], wbuf.at[d, share, :], wf_ss.at[d, k], wf_rs.at[d, k], {"context": lax.rem(c + k, nc)})
            for k in range(1, nc)
        ])
    for d in range(1, 2):
        for cp in wfs[d - 1]:
            cp.wait()
        project(d)
        sent += scatter(d)
    for cp in ags + gbs:
        cp.wait()
    ag_all[t] = ag_own[...]
    grad = jnp.zeros((16, LW), F32)
    for s in range(nt):
        grad = grad + dot(ag_all[s].astype(BF), g_s[s * L : (s + 1) * L, :])
    comb[:, 0:LW] = grad
    acc = gb_own[:, own_part]
    for e in range(1, nt):
        acc = acc + gb_in[e]
    comb[:, LW : LW + part] = acc
    ccs = [copy(comb, comb_c.at[k], cc_ss.at[k], cc_rs.at[k], {"context": lax.rem(c + k, nc)}) for k in range(1, nc)]
    for d in range(2, nf):
        for cp in wfs[d - 1]:
            cp.wait()
        project(d)
        sent += scatter(d)
        if d == 2:
            for cp in ccs:
                cp.wait()
            acc = comb[...]
            for k in range(1, nc):
                acc = acc + comb_c[k]
            comb2[...] = acc
            cfs = [copy(comb2, comb_f.at[k], cf_ss.at[k], cf_rs.at[k], {"fsdp": lax.rem(f + k, nf)}) for k in range(1, nf)]
    for cp in cfs:
        cp.wait()
    acc = comb2[...]
    for k in range(1, nf):
        acc = acc + comb_f[k]
    ga_ref[...] = acc[:, 0:LW]
    fin[t] = acc[:, LW:]
    fins = [copy(fin.at[t], fin.at[t], fin_ss.at[e], fin_rs.at[e], {"tensor": tp(e)}) for e in range(1, nt)]
    scale_col = dot(jnp.broadcast_to(scale_row, (8, L)), jnp.full((8, 128), 0.125, F32), 0, 0, HI)[:, 0:1]
    for d in range(nf):
        for cp in sent[d * (nt - 1) : (d + 1) * (nt - 1)]:
            cp.wait()
        cols = pl.ds(pl.multiple_of(lax.rem(f + nf - d, nf) * W, 128), W)
        acc = rs_send[d, own_rows, :].astype(F32)
        for e in range(1, nt):
            acc = acc + rs_recv[d, e - 1].astype(F32)
        acc = acc + 2.0 * dot(ad16, up_ref[:, cols], 0, 0)
        mixed_ref[:, cols] = (scale_col * acc).astype(BF)
    for cp in fins:
        cp.wait()
    for s in range(nt):
        gb_ref[:, s * part : (s + 1) * part] = fin[s]


def shards(x, bc, z, dt, taps, bias, step_bias, rate, skip, gain, w, down, up, cot):
    nt, nf, nc = lax.axis_size("tensor"), lax.axis_size("fsdp"), lax.axis_size("context")
    L, full = x.shape[1], x.shape[2]
    LW, hl, W, M = gain.shape[0], step_bias.shape[0], w.shape[1], cot.shape[2]
    BC = bc.shape[2]
    N = BC // 2
    HR = -(-hl // 8) * 8
    T = nt * L
    part = M // nt
    hp = jnp.pad(jnp.stack([step_bias, rate, skip]), ((0, 5), (0, 128 - hl)))
    dt = jnp.pad(dt[0], ((0, 0), (0, 128 - dt.shape[2])))
    vm = pl.BlockSpec(memory_space=pltpu.VMEM)
    hbm = pl.BlockSpec(memory_space=pl.ANY)
    V = pltpu.VMEM
    D = pltpu.SemaphoreType.DMA
    scratch = [
        V((16, full), BF), V((16, BC), BF), V((nt - 1, L, LW), BF), V((T, LW), BF), V((T, LW), BF),
        V((T, BC), BF), V((T, 128), BF), V((nf, LW, W), BF), V((T, 128), F32), V((T, 128), F32),
        V((nt, HR, L), F32), V((nt, HR, L), F32),
        V((nt, N + 8, LW), F32), V((N + 8, LW), F32), V((nc, N + 8, LW), F32), V((N, LW), F32),
        V((128, LW), F32), V((T, LW), F32), V((T, LW), BF), V((nt, 24, L), F32), V((nt, 24, L), F32),
        V((16, L), F32), V((nt, 16, L), F32), V((16, M), F32), V((nt, 16, part), F32),
        V((16, LW + part), F32), V((nc, 16, LW + part), F32), V((16, LW + part), F32), V((nf, 16, LW + part), F32),
        V((nt, 16, part), F32), V((nf, T, W), BF), V((nf, nt - 1, L, W), BF),
        D((2,)), D((2,)), D((nt,)), D((nt,)), D((nt,)), D((nt,)), D((nt,)), D((nt,)), D((nt,)), D((nt,)),
        D((nf,)), D((nf,)), D((nf, nc)), D((nf, nc)), D((nc,)), D((nc,)),
        D((nt,)), D((nt,)), D((nt,)), D((nt,)), D((nt,)), D((nt,)), D((nc,)), D((nc,)), D((nf,)), D((nf,)),
        D((nt,)), D((nt,)), D((nf, nt)), D((nf, nt)), D((2,)),
    ]
    mixed, ga, gb = pl.pallas_call(
        functools.partial(kernel, nt, nf, nc, hl),
        out_shape=(
            jax.ShapeDtypeStruct((L, M), BF),
            jax.ShapeDtypeStruct((16, LW), F32),
            jax.ShapeDtypeStruct((16, M), F32),
        ),
        in_specs=[vm, vm, hbm, vm, vm, vm, vm, vm, hbm, vm, vm, vm],
        out_specs=(vm, vm, vm),
        scratch_shapes=scratch,
        compiler_params=pltpu.CompilerParams(
            collective_id=0, has_side_effects=True, vmem_limit_bytes=62 * 1024 * 1024
        ),
    )(x[0], bc[0], z[0], dt, taps, bias[None], hp, gain[None], w, down.T, up, cot[0])
    return mixed[None], ga.T, gb


def solution(mesh):
    tokens = P("fsdp", ("context", "tensor"), None)
    placed = (
        tokens, tokens, tokens, tokens, P(), P(), P("tensor"), P("tensor"), P("tensor"), P("tensor"),
        P("tensor", "fsdp"), P("tensor", None), P(), tokens,
    )
    return jax.shard_map(
        shards, mesh=mesh, in_specs=placed, out_specs=(tokens, P("tensor", None), P()), check_vma=False
    )
```

```python
import functools
import math

import jax
import jax.numpy as jnp
from jax import lax
from jax.experimental import pallas as pl
from jax.experimental.pallas import tpu as pltpu
from jax.sharding import PartitionSpec as P

EPS = 1e-05
MESH = pl.DeviceIdType.MESH
HI = lax.Precision.HIGHEST
BF = jnp.bfloat16
F32 = jnp.float32


def dot(a, b, ca=1, cb=0, precision=None):
    return lax.dot_general(
        a, b, (((ca,), (cb,)), ((), ())), preferred_element_type=F32, precision=precision
    )


def iota(shape, dim):
    return lax.broadcasted_iota(jnp.int32, shape, dim)


def kernel(
    nt, nf, nc, hl,
    x_ref, bc_ref, z_ref, dt_ref, taps_ref, bias_ref, sb_ref, dr_ref, sk_ref, gain_ref, w_ref, down_ref, up_ref, cot_ref,
    mixed_ref, ga_ref, gb_ref,
    halo_x, halo_bc, x_send, x_all, z_all, bc_all, dt_all, wbuf, a_s, step_s, at_s, stept_s,
    stl, msg, st_in, inc_s, e_s, y_s, g_s, adx, ad_in, ag_own, ag_all, gb_own, gb_in, comb, comb_c, comb2, comb_f,
    fin, rs_send, rs_recv,
    h_ss, h_rs, dt_ss, dt_rs, bc_ss, bc_rs, x_ss, x_rs, z_ss, z_rs, w_ss, w_rs, wf_ss, wf_rs, st_ss, st_rs,
    ad_ss, ad_rs, ag_ss, ag_rs, ga_ss, ga_rs, cc_ss, cc_rs, cf_ss, cf_rs, fin_ss, fin_rs, r_ss, r_rs, loc,
):
    t = lax.axis_index("tensor")
    f = lax.axis_index("fsdp")
    c = lax.axis_index("context")
    L = x_ref.shape[0]
    LW = x_all.shape[1]
    W = w_ref.shape[1]
    N = bc_ref.shape[1] // 2
    R = w_ref.shape[0] // nc
    HS = LW // hl
    idx = c * nt + t
    total = nc * nt

    def tp(e):
        return lax.rem(t + e, nt)

    def place(i):
        return {"context": i // nt, "tensor": lax.rem(i, nt)}

    def copy(src, dst, ss, rs, dev):
        cp = pltpu.make_async_remote_copy(
            src_ref=src, dst_ref=dst, send_sem=ss, recv_sem=rs, device_id=dev, device_id_type=MESH
        )
        cp.start()
        return cp

    nxt, prv = lax.rem(idx + 1, total), lax.rem(idx + total - 1, total)
    bar = pltpu.get_barrier_semaphore()
    greet = [{"tensor": tp(e)} for e in range(1, nt)]
    greet += [{"fsdp": lax.rem(f + d, nf)} for d in range(1, nf)]
    greet += [{"context": lax.rem(c + k, nc)} for k in range(1, nc)]
    greet += [place(nxt), place(prv)]
    for dev in greet:
        pl.semaphore_signal(bar, inc=1, device_id=dev, device_id_type=MESH)
    pl.semaphore_wait(bar, len(greet))
    sent = []

    h1 = copy(x_ref.at[L - 16 : L, :], halo_x, h_ss.at[0], h_rs.at[0], place(nxt))
    h2 = copy(bc_ref.at[L - 16 : L, :], halo_bc, h_ss.at[1], h_rs.at[1], place(nxt))
    own_rows = pl.ds(pl.multiple_of(t * L, L), L)
    dts = [copy(dt_ref, dt_all.at[t], dt_ss.at[e], dt_rs.at[e], {"tensor": tp(e)}) for e in range(1, nt)]
    share = pl.ds(pl.multiple_of(c * R, 16), R)
    ws = [
        copy(w_ref.at[share, :], wbuf.at[d, share, :], w_ss.at[d], w_rs.at[d], {"fsdp": lax.rem(f + d, nf)})
        for d in range(1, nf)
    ]
    own_w = pltpu.make_async_copy(w_ref, wbuf.at[0], loc.at[0])
    own_w.start()
    own_cols = pl.ds(pl.multiple_of(t * LW, 128), LW)
    own_z = pltpu.make_async_copy(z_ref.at[:, own_cols], z_all.at[own_rows, :], loc.at[1])
    own_z.start()
    dt_all[t] = dt_ref[...]

    def send_gate(e):
        cols = pl.ds(pl.multiple_of(tp(e) * LW, 128), LW)
        return copy(z_ref.at[:, cols], z_all.at[own_rows, :], z_ss.at[e], z_rs.at[e], {"tensor": tp(e)})

    zs = [send_gate(1)]
    h1.wait()
    h2.wait()
    live = (idx > 0).astype(F32)

    def conv(src, halo, col, tap_col):
        lanes = pl.ds(col, 128)
        wide = pl.ds(tap_col, 128)
        ext = jnp.concatenate([halo[8:16, lanes].astype(F32) * live, src[:, lanes].astype(F32)], axis=0)
        acc = bias_ref[:, wide] + taps_ref[0:1, wide] * ext[5 : 5 + L]
        for k in range(1, 4):
            acc = acc + taps_ref[k : k + 1, wide] * ext[5 + k : 5 + k + L]
        return (acc / (1.0 + jnp.exp(-acc))).astype(BF)

    wide0 = x_ref.shape[1]
    for j in range(2 * N // 128):
        bc_all[own_rows, j * 128 : (j + 1) * 128] = conv(bc_ref, halo_bc, j * 128, wide0 + j * 128)
    bcs = [
        copy(bc_all.at[own_rows, :], bc_all.at[own_rows, :], bc_ss.at[e], bc_rs.at[e], {"tensor": tp(e)})
        for e in range(1, nt)
    ]
    xs = []

    def conv_group(e, store):
        base = tp(e) * LW

        def lap(j, carry):
            col = pl.multiple_of(base + j * 128, 128)
            store(pl.ds(pl.multiple_of(j * 128, 128), 128), conv(x_ref, halo_x, col, col))
            return carry

        lax.fori_loop(0, LW // 128, lap, 0)

    for e in range(1, nt):
        def put(lanes, val, e=e):
            x_send[e - 1, :, lanes] = val

        conv_group(e, put)
        xs.append(copy(x_send.at[e - 1], x_all.at[own_rows, :], x_ss.at[e], x_rs.at[e], {"tensor": tp(e)}))
    for e in range(2, nt):
        zs.append(send_gate(e))

    def put_own(lanes, val):
        x_all[own_rows, lanes] = val

    conv_group(0, put_own)
    e_s[...] = (iota((128, LW), 1) // HS == iota((128, LW), 0)).astype(F32)
    spread16 = e_s[...].astype(BF)

    def spread(rows):
        return dot(jnp.broadcast_to(rows, (8, 128)), e_s[...], precision=HI)

    for cp in dts:
        cp.wait()
    HR = at_s.shape[1]
    HA = dt_ref.shape[0]
    sel = ((iota((HA, 128), 0) == iota((HA, 128), 1) + t * hl) & (iota((HA, 128), 1) < hl)).astype(BF)
    sel_t = ((iota((HR, HA), 1) == iota((HR, HA), 0) + t * hl) & (iota((HR, HA), 0) < hl)).astype(BF)
    eye = (iota((HR, 128), 0) == iota((HR, 128), 1)).astype(F32)
    place_head = (iota((hl, 128), 0) == iota((hl, 128), 1)).astype(F32)
    hp = [
        dot(jnp.broadcast_to(v[...], (8, hl)), place_head, precision=HI)[0:1, :] for v in (sb_ref, dr_ref, sk_ref)
    ]
    hp_t = [dot(eye, jnp.broadcast_to(v, (8, 128)), 1, 1, HI)[:, 0:1] for v in hp[0:2]]
    tri = (iota((L, L), 0) >= iota((L, L), 1)).astype(F32)

    def softplus(v):
        return jnp.maximum(v, 0.0) + jnp.log1p(jnp.exp(-jnp.abs(v)))

    for b in range(nt):
        rows = slice(b * L, (b + 1) * L)
        raw = dt_all[b]
        step = softplus(dot(raw, sel, 0, 0) + hp[0])
        step_s[rows, :] = step
        a_s[rows, :] = dot(tri, -step * jnp.exp(hp[1]), precision=HI)
        step_t = softplus(dot(sel_t, raw) + hp_t[0])
        stept_s[b] = step_t
        at_s[b] = dot(-step_t * jnp.exp(hp_t[1]), tri, 1, 1, HI)
    for cp in bcs:
        cp.wait()
    for cp in xs:
        cp.wait()

    state = jnp.zeros((N, LW), F32)
    before = jnp.zeros((1, 128), F32)
    for b in range(nt):
        rows = slice(b * L, (b + 1) * L)
        stl[b, 0:N, :] = state
        stl[b, N : N + 8, :] = spread(jnp.exp(before))
        a = a_s[rows, :]
        last = a[L - 1 : L, :]
        weight = (jnp.exp(last - a) * step_s[rows, :]).astype(BF)
        xw = (x_all[rows, :].astype(F32) * dot(weight, spread16)).astype(BF)
        state = spread(jnp.exp(last))[0:1, :] * state + dot(bc_all[rows, 0:N], xw, 0, 0)
        before = before + last
    msg[0:N, :] = state
    msg[N : N + 8, :] = spread(before)
    sts = [
        copy(msg, st_in.at[c], st_ss.at[k], st_rs.at[k], {"context": lax.rem(c + k, nc)})
        for k in range(1, nc)
    ]

    left = iota((L, 2 * HS), 1) < HS

    def inner(b, carry):
        rows = pl.ds(pl.multiple_of(b * L, L), L)
        gram = dot(bc_all[rows, N : 2 * N], bc_all[rows, 0:N], 1, 1)
        gram = jnp.where(iota((L, L), 0) >= iota((L, L), 1), gram, 0.0)
        a = a_s[rows, :]
        at = at_s[b]
        stt = stept_s[b]
        for pair in range(hl // 2):
            lanes = slice(pair * 2 * HS, (pair + 1) * 2 * HS)
            xp = x_all[rows, lanes]
            out = []
            for h in (2 * pair, 2 * pair + 1):
                gap = jnp.minimum(a[:, h : h + 1] - at[h : h + 1, :], 0.0)
                m = (jnp.exp(gap) * gram * stt[h : h + 1, :]).astype(BF)
                out.append(dot(m, xp))
            y_s[rows, lanes] = jnp.where(left, out[0], out[1])
        return carry

    lax.fori_loop(0, nt, inner, 0)

    for cp in sts:
        cp.wait()
    inc_s[...] = jnp.zeros_like(inc_s)

    def chain(k, carry):
        inc_s[...] = jnp.exp(st_in[k, N : N + 1, :]) * inc_s[...] + st_in[k, 0:N, :]
        return carry

    lax.fori_loop(0, c, chain, 0)
    for cp in zs:
        cp.wait()
    own_z.wait()
    skip = spread(hp[2])[0:1, :]
    ones = jnp.ones((8, LW), BF)

    def gate(b, carry):
        rows = pl.ds(pl.multiple_of(b * L, L), L)
        start = (stl[b, 0:N, :] + stl[b, N : N + 1, :] * inc_s[...]).astype(BF)
        reach = dot(jnp.exp(a_s[rows, :]).astype(BF), spread16)
        y = y_s[rows, :] + reach * dot(bc_all[rows, N : 2 * N], start)
        y = y + skip * x_all[rows, :].astype(F32)
        z = z_all[rows, :].astype(F32)
        g = y * (z / (1.0 + jnp.exp(-z)))
        out = (g * gain_ref[...]).astype(BF)
        g_s[rows, :] = out
        adx[b, 0:16, :] = dot(down_ref[...], out, 1, 1)
        adx[b, 16:24, :] = dot(ones, (g * g).astype(BF), 1, 1)
        return carry

    lax.fori_loop(0, nt, gate, 0)
    ads = [copy(adx.at[tp(e)], ad_in.at[e], ad_ss.at[e], ad_rs.at[e], {"tensor": tp(e)}) for e in range(1, nt)]

    half = (nt * L) // 2

    def project(d):
        def lap(i, carry):
            rows = pl.ds(pl.multiple_of(i * half, half), half)
            rs_send[d, rows, :] = dot(g_s[rows, :], wbuf[d]).astype(BF)
            return carry

        lax.fori_loop(0, 2, lap, 0)

    def scatter(d):
        return [
            copy(
                rs_send.at[d, pl.ds(pl.multiple_of(tp(e) * L, L), L), :],
                rs_recv.at[d, e - 1], r_ss.at[d, e], r_rs.at[d, e], {"tensor": tp(e)},
            )
            for e in range(1, nt)
        ]

    own_w.wait()
    project(0)
    for cp in ads:
        cp.wait()
    red = adx[t]
    for e in range(1, nt):
        red = red + ad_in[e]
    scale_row = lax.rsqrt(red[16:17, :] / (LW * nt) + EPS)
    ad16 = red[0:16, :].astype(BF)
    factor = 2.0 / math.sqrt(L * nt * nc * nf)
    cot = cot_ref[...]
    ag_own[...] = factor * scale_row * dot(up_ref[...], cot, 1, 1)
    ags = [copy(ag_own, ag_all.at[t], ag_ss.at[e], ag_rs.at[e], {"tensor": tp(e)}) for e in range(1, nt)]
    gb_own[...] = dot((factor * scale_row * ad16.astype(F32)).astype(BF), cot)
    part = gb_own.shape[1] // nt
    own_part = pl.ds(pl.multiple_of(t * part, 128), part)
    gbs = [
        copy(
            gb_own.at[:, pl.ds(pl.multiple_of(tp(e) * part, 128), part)],
            gb_in.at[e], ga_ss.at[e], ga_rs.at[e], {"tensor": tp(e)},
        )
        for e in range(1, nt)
    ]
    sent += scatter(0)
    for cp in ags + gbs:
        cp.wait()
    ag_all[t] = ag_own[...]
    grad = jnp.zeros((16, LW), F32)
    for s in range(nt):
        grad = grad + dot(ag_all[s].astype(BF), g_s[s * L : (s + 1) * L, :])
    comb[:, 0:LW] = grad
    acc = gb_own[:, own_part]
    for e in range(1, nt):
        acc = acc + gb_in[e]
    comb[:, LW : LW + part] = acc
    ccs = [copy(comb, comb_c.at[k], cc_ss.at[k], cc_rs.at[k], {"context": lax.rem(c + k, nc)}) for k in range(1, nc)]
    wfs = []
    for d in range(1, nf):
        ws[d - 1].wait()
        wfs.append([
            copy(wbuf.at[d, share, :], wbuf.at[d, share, :], wf_ss.at[d, k], wf_rs.at[d, k], {"context": lax.rem(c + k, nc)})
            for k in range(1, nc)
        ])
    for cp in ccs:
        cp.wait()
    acc = comb[...]
    for k in range(1, nc):
        acc = acc + comb_c[k]
    comb2[...] = acc
    cfs = [copy(comb2, comb_f.at[k], cf_ss.at[k], cf_rs.at[k], {"fsdp": lax.rem(f + k, nf)}) for k in range(1, nf)]
    for d in range(1, nf):
        for cp in wfs[d - 1]:
            cp.wait()
        project(d)
        sent += scatter(d)
    for cp in cfs:
        cp.wait()
    acc = comb2[...]
    for k in range(1, nf):
        acc = acc + comb_f[k]
    ga_ref[...] = acc[:, 0:LW]
    fin[t] = acc[:, LW:]
    fins = [copy(fin.at[t], fin.at[t], fin_ss.at[e], fin_rs.at[e], {"tensor": tp(e)}) for e in range(1, nt)]
    scale_col = dot(jnp.broadcast_to(scale_row, (8, L)), jnp.full((8, 128), 0.125, F32), 0, 0, HI)[:, 0:1]
    for d in range(nf):
        for cp in sent[d * (nt - 1) : (d + 1) * (nt - 1)]:
            cp.wait()
        cols = pl.ds(pl.multiple_of(lax.rem(f + nf - d, nf) * W, 128), W)
        acc = rs_send[d, own_rows, :].astype(F32)
        for e in range(1, nt):
            acc = acc + rs_recv[d, e - 1].astype(F32)
        acc = acc + 2.0 * dot(ad16, up_ref[:, cols], 0, 0)
        mixed_ref[:, cols] = (scale_col * acc).astype(BF)
    for cp in fins:
        cp.wait()
    for s in range(nt):
        gb_ref[:, s * part : (s + 1) * part] = fin[s]


def shards(x, bc, z, dt, taps, bias, step_bias, rate, skip, gain, w, down, up, cot):
    nt, nf, nc = lax.axis_size("tensor"), lax.axis_size("fsdp"), lax.axis_size("context")
    L, full = x.shape[1], x.shape[2]
    LW, hl, W, M = gain.shape[0], step_bias.shape[0], w.shape[1], cot.shape[2]
    BC = bc.shape[2]
    N = BC // 2
    HR = -(-hl // 8) * 8
    T = nt * L
    part = M // nt
    dt = dt[0].T
    vm = pl.BlockSpec(memory_space=pltpu.VMEM)
    hbm = pl.BlockSpec(memory_space=pl.ANY)
    V = pltpu.VMEM
    D = pltpu.SemaphoreType.DMA
    scratch = [
        V((16, full), BF), V((16, BC), BF), V((nt - 1, L, LW), BF), V((T, LW), BF), V((T, LW), BF),
        V((T, BC), BF), V((nt,) + dt.shape, BF), V((nf, LW, W), BF), V((T, 128), F32), V((T, 128), F32),
        V((nt, HR, L), F32), V((nt, HR, L), F32),
        V((nt, N + 8, LW), F32), V((N + 8, LW), F32), V((nc, N + 8, LW), F32), V((N, LW), F32),
        V((128, LW), F32), V((T, LW), F32), V((T, LW), BF), V((nt, 24, L), F32), V((nt, 24, L), F32),
        V((16, L), F32), V((nt, 16, L), F32), V((16, M), F32), V((nt, 16, part), F32),
        V((16, LW + part), F32), V((nc, 16, LW + part), F32), V((16, LW + part), F32), V((nf, 16, LW + part), F32),
        V((nt, 16, part), F32), V((nf, T, W), BF), V((nf, nt - 1, L, W), BF),
        D((2,)), D((2,)), D((nt,)), D((nt,)), D((nt,)), D((nt,)), D((nt,)), D((nt,)), D((nt,)), D((nt,)),
        D((nf,)), D((nf,)), D((nf, nc)), D((nf, nc)), D((nc,)), D((nc,)),
        D((nt,)), D((nt,)), D((nt,)), D((nt,)), D((nt,)), D((nt,)), D((nc,)), D((nc,)), D((nf,)), D((nf,)),
        D((nt,)), D((nt,)), D((nf, nt)), D((nf, nt)), D((2,)),
    ]
    mixed, ga, gb = pl.pallas_call(
        functools.partial(kernel, nt, nf, nc, hl),
        out_shape=(
            jax.ShapeDtypeStruct((L, M), BF),
            jax.ShapeDtypeStruct((16, LW), F32),
            jax.ShapeDtypeStruct((16, M), F32),
        ),
        in_specs=[vm, vm, hbm, vm, vm, vm, vm, vm, vm, vm, hbm, vm, vm, vm],
        out_specs=(vm, vm, vm),
        scratch_shapes=scratch,
        compiler_params=pltpu.CompilerParams(
            collective_id=0, has_side_effects=True, vmem_limit_bytes=62 * 1024 * 1024
        ),
    )(x[0], bc[0], z[0], dt, taps, bias[None], step_bias[None], rate[None], skip[None], gain[None], w, down.T, up, cot[0])
    return mixed[None], ga.T, gb


def solution(mesh):
    tokens = P("fsdp", ("context", "tensor"), None)
    placed = (
        tokens, tokens, tokens, tokens, P(), P(), P("tensor"), P("tensor"), P("tensor"), P("tensor"),
        P("tensor", "fsdp"), P("tensor", None), P(), tokens,
    )
    return jax.shard_map(
        shards, mesh=mesh, in_specs=placed, out_specs=(tokens, P("tensor", None), P()), check_vma=False
    )
```
